512 devices in a mesh: grp: 8 (over y), row: 64 (over z, x, core).
Axes of the slice: x: 4, y: 8, z: 8, core: 2. Of those that a mesh axis runs over, the one named last changes fastest.
Arguments:
- embeddings: bfloat16 [262144, 768], P(('grp', 'row')), may hold values from -2000 to 2000
Outputs:
- whitened: bfloat16 [262144, 768], P(('grp', 'row'))
- energy: float32 [], replicated
The draws below stay inside these ranges and needn't reach their ends.
All inputs are finite; a program needn't handle non-finite values.
Results may differ from the reference program's by a relative error of at most 0.0007.
The reference program's roundings to bfloat16 on the way (of `transform` and `centered`) count: a program that leaves them out, or rounds other values in their place, can miss the bound.
Values may be sent and summed in bfloat16 or wider, within the bound.
No kernel may reach another device: no remote copies, remote signals or barrier semaphores. Data moves between devices by JAX's collectives and lax.ppermute only.
A program may use at most 64 MiB of HBM per device.

```python
import math
import jax
import jax.numpy as jnp
from jax import lax

D = 768
ROW_DEV = 512
ITERS = 4
ROWS = 262144


def draw_embeddings(key, part):
    keys = [jax.random.fold_in(key, 101 + index) for index in range(8)]
    base = jnp.clip(jax.random.normal(keys[0], (ROWS, D), jnp.float32), -4.0, 4.0)
    top_log = math.log(10.0)
    colscale = jnp.exp(jax.random.uniform(keys[1], (1, D), jnp.float32, 0.0, top_log))
    position = jnp.arange(ROWS, dtype=jnp.float32)[:, None] / ROWS
    rowscale = jnp.exp(jax.random.uniform(keys[2], (ROWS, 1), jnp.float32, 0.0, math.log(10.0))) * (1.0 + 2.0 * position)
    spread = base * colscale
    mixed = spread + 0.6 * jnp.roll(spread, 1, axis=1) + 0.4 * jnp.roll(spread, 37, axis=1)
    offset = jax.random.normal(keys[3], (1, D), jnp.float32) * colscale
    values = rowscale * mixed + 4.0 * offset
    return jnp.clip(values, -2000.0, 2000.0).astype(jnp.bfloat16)


def setup_inputs(seed: int = 0) -> dict:
    splits = jax.random.split(jax.random.key(seed), 2)
    return {
        "embeddings": draw_embeddings(jax.random.fold_in(splits[1], 71), 0),
    }


def reference(embeddings):
    rows_total = embeddings.shape[0]
    width = embeddings.shape[1]
    blocks = embeddings.reshape(-1, ROW_DEV, width)

    def accumulate(carry, block):
        second, colsum = carry
        second = second + jnp.dot(block.T, block, preferred_element_type=jnp.float32)
        colsum = colsum + lax.optimization_barrier(jnp.sum(block.astype(jnp.float32), axis=0))
        return ((second, colsum), None)
    start = (jnp.zeros((width, width), jnp.float32), jnp.zeros((width,), jnp.float32))
    (second, colsum), unused = lax.scan(accumulate, start, blocks)
    mean = colsum / rows_total
    cov = second / rows_total - mean[:, None] * mean[None, :]
    fro = jnp.sqrt(jnp.sum(cov * cov) + 1e-06)
    scaled = cov / fro
    eye = jnp.eye(width, dtype=jnp.float32)
    hp = lax.Precision.HIGHEST
    iterate = 1.5 * eye - 0.5 * scaled
    for step in range(ITERS - 1):
        prod = jnp.dot(jnp.dot(jnp.dot(scaled, iterate, precision=hp), iterate, precision=hp), iterate, precision=hp)
        iterate = 1.5 * iterate - 0.5 * prod
    transform = (iterate / jnp.sqrt(fro)).astype(jnp.bfloat16)

    def apply(block):
        centered = (block.astype(jnp.float32) - mean).astype(jnp.bfloat16)
        product = jnp.dot(centered, transform.T, preferred_element_type=jnp.float32)
        return (product.astype(jnp.bfloat16), jnp.sum(product * product))
    outputs, sums = lax.map(apply, blocks)
    whitened = outputs.reshape(rows_total, width)
    energy = jnp.sum(sums) / (rows_total * width)
    return (whitened, energy)
```

```python
import functools

import jax
import jax.numpy as jnp
from jax import lax
from jax.experimental import pallas as pl
from jax.experimental.pallas import tpu as pltpu
from jax.sharding import Mesh
from jax.sharding import PartitionSpec as P

ITERS = 4
AXES = ("grp", "row_0", "row_1", "row_2")
LANES = 128
TILE = 256
F32 = jnp.float32
BF16 = jnp.bfloat16


def layout(width):
    nb = width // LANES
    off = {}
    at = 0
    for i in range(nb):
        for j in range(i + 1, nb):
            off[i, j] = at
            at += LANES
    merged = {}
    for i in range(0, nb, 2):
        merged[i] = at
        at += LANES
    return nb, off, merged, at


def upper(shape):
    r = lax.broadcasted_iota(jnp.int32, shape, 0)
    c = lax.broadcasted_iota(jnp.int32, shape, 1)
    return r <= c, r == c


def gram_kernel(e_ref, o_ref):
    width = e_ref.shape[1]
    nb, off, merged, tail = layout(width)
    e = e_ref[...]
    keep, diag = upper((LANES, LANES))
    diagonal = {}
    lines = []
    for big in range(0, width, TILE):
        g = lax.dot_general(
            e[:, big : big + TILE], e[:, big:], (((0,), (0,)), ((), ())), preferred_element_type=F32
        )
        for i in range(big // LANES, (big + TILE) // LANES):
            r = i * LANES - big
            for j in range(i, nb):
                block = g[r : r + LANES, j * LANES - big : (j + 1) * LANES - big]
                if i == j:
                    diagonal[i] = block
                else:
                    o_ref[off[i, j] : off[i, j] + LANES, :] = block
        i = big // LANES
        a, b = diagonal[i], diagonal[i + 1]
        o_ref[merged[i] : merged[i] + LANES, :] = jnp.where(keep, a, b)
        lines.append(jnp.sum(jnp.where(diag, b, 0.0), axis=0, keepdims=True))
    colsum = jnp.sum(e.astype(F32), axis=0, keepdims=True)
    o_ref[tail:, :] = jnp.zeros((o_ref.shape[0] - tail, LANES), F32)
    for k in range(nb):
        o_ref[tail + k : tail + k + 1, :] = colsum[:, k * LANES : (k + 1) * LANES]
    for k, line in enumerate(lines):
        o_ref[tail + nb + k : tail + nb + k + 1, :] = line


def total_kernel(piece, x_ref, o_ref):
    period = 8 * piece
    groups = x_ref.shape[0] // period
    acc = jnp.sum(x_ref[...].reshape(groups, period, LANES), axis=0)
    for shift in (piece, 2 * piece, 4 * piece):
        acc = acc + jnp.concatenate([acc[period - shift :], acc[: period - shift]], axis=0)
    for g in range(groups):
        o_ref[g * period : (g + 1) * period, :] = acc


def split(x):
    hi = x.astype(BF16)
    lo = (x - hi.astype(F32)).astype(BF16)
    return hi, lo


def whiten_kernel(rows_total, e_ref, p_ref, o_ref, en_ref, s_ref, r_ref, q_ref, sh, sl, ah, al, bh, bl, w_ref):
    rows_dev, width = e_ref.shape
    nb, off, merged, tail = layout(width)
    inv = 1.0 / rows_total
    keep, diag = upper((LANES, LANES))
    means = [p_ref[tail + k : tail + k + 1, :] * inv for k in range(nb)]
    down = [jnp.transpose(jnp.broadcast_to(m, (LANES, LANES))) for m in means]

    squares = jnp.zeros((LANES, LANES), F32)
    for i in range(nb):
        for j in range(i, nb):
            if i != j:
                block = p_ref[off[i, j] : off[i, j] + LANES, :]
            else:
                base = i - i % 2
                packed = p_ref[merged[base] : merged[base] + LANES, :]
                mirror = jnp.transpose(packed)
                if i == base:
                    block = jnp.where(keep, packed, mirror)
                else:
                    line = p_ref[tail + nb + base // 2 : tail + nb + base // 2 + 1, :]
                    block = jnp.where(diag, line, jnp.where(keep, mirror, packed))
            cov = block * inv - down[i] * means[j]
            squares = squares + (cov * cov) * (1.0 if i == j else 2.0)
            s_ref[i * LANES : (i + 1) * LANES, j * LANES : (j + 1) * LANES] = cov
    total = jnp.sum(jnp.sum(squares, axis=0, keepdims=True), axis=1, keepdims=True)
    fro = jnp.sqrt(total + 1e-06)
    rescale = 1.0 / fro
    for i in range(nb):
        for j in range(i, nb):
            at = (slice(i * LANES, (i + 1) * LANES), slice(j * LANES, (j + 1) * LANES))
            s = s_ref[at] * rescale
            s_ref[at] = s
            sh[at], sl[at] = split(s)
            if i != j:
                turned = jnp.transpose(s)
                ta = (at[1], at[0])
                sh[ta], sl[ta] = split(turned)
                if i // (TILE // LANES) == j // (TILE // LANES):
                    s_ref[ta] = turned

    nt = width // TILE
    pairs = [(i, j) for i in range(nt) for j in range(i, nt)]

    def span(i):
        return slice(i * TILE, (i + 1) * TILE)

    def dot(a, b):
        return jnp.dot(a, b, preferred_element_type=F32)

    def product(xh, xl, yh, yl, i, j):
        a, b = span(i), span(j)
        return dot(xh[a, :], yh[:, b]) + (dot(xh[a, :], yl[:, b]) + dot(xl[a, :], yh[:, b]))

    def put(h_ref, l_ref, i, j, x):
        h_ref[span(i), span(j)], l_ref[span(i), span(j)] = split(x)
        if i != j:
            h_ref[span(j), span(i)], l_ref[span(j), span(i)] = split(jnp.transpose(x))

    def double_step(t_ref, th, tl, x_ref):
        for i, j in pairs:
            at = (span(i), span(j))
            t2 = product(th, tl, th, tl, i, j)
            t = t_ref[at]
            put(ah, al, i, j, t2)
            put(bh, bl, i, j, 0.0625 * t2 - 0.5625 * t)
            x_ref[at] = 1.6875 * t2 - 2.4375 * t
        for i, j in pairs:
            at = (span(i), span(j))
            x_ref[at] = x_ref[at] + product(ah, al, bh, bl, i, j)

    double_step(s_ref, sh, sl, r_ref)
    for i, j in pairs:
        put(ah, al, i, j, r_ref[span(i), span(j)])
    for i, j in pairs:
        at = (span(i), span(j))
        put(bh, bl, i, j, 4.5 * r_ref[at] + product(ah, al, ah, al, i, j))
    for i, j in pairs:
        at = (span(i), span(j))
        q_ref[at] = 5.0625 * s_ref[at] + product(sh, sl, bh, bl, i, j)
    for i, j in pairs:
        put(sh, sl, i, j, q_ref[span(i), span(j)])
    double_step(q_ref, sh, sl, q_ref)
    for i, j in pairs:
        put(ah, al, i, j, r_ref[span(i), span(j)])
        put(bh, bl, i, j, q_ref[span(i), span(j)])
    root = lax.rsqrt(fro)
    one = upper((TILE, TILE))[1]
    for i, j in pairs:
        at = (span(i), span(j))
        z = 2.25 * (r_ref[at] + q_ref[at]) + product(ah, al, bh, bl, i, j)
        if i == j:
            z = z + jnp.where(one, 5.0625, 0.0)
        w = (z * root).astype(BF16)
        w_ref[at] = w
        if i != j:
            w_ref[span(j), span(i)] = jnp.transpose(w.astype(F32)).astype(BF16)

    acc = jnp.zeros((TILE, TILE), F32)
    for i, j in pairs:
        g = dot(w_ref[span(i), :], w_ref[:, span(j)])
        acc = acc + g * s_ref[span(i), span(j)] * (1.0 if i == j else 2.0)
    trace = jnp.sum(jnp.sum(acc, axis=0, keepdims=True), axis=1, keepdims=True)
    en_ref[...] = trace * fro * (1.0 / width)

    mean = jnp.concatenate(means, axis=1)
    for r in range(0, rows_dev, TILE):
        c = (e_ref[r : r + TILE, :].astype(F32) - mean).astype(BF16)
        o_ref[r : r + TILE, :] = dot(c, w_ref[...]).astype(BF16)


def local(embeddings):
    rows_dev, width = embeddings.shape
    peers = lax.axis_size(AXES)
    rows_total = rows_dev * peers
    _, _, _, tail = layout(width)
    piece = -(-(tail + 16) // peers)
    rows = piece * peers
    packed_type = jax.ShapeDtypeStruct((rows, LANES), F32)
    vmem = pl.BlockSpec(memory_space=pltpu.VMEM)

    def exchange(x):
        x = x.reshape(peers, 1, piece * LANES)
        return lax.all_to_all(x, AXES, 0, 0, tiled=True).reshape(rows, LANES)

    packed = pl.pallas_call(gram_kernel, out_shape=packed_type, in_specs=[vmem], out_specs=vmem, name="gram")(embeddings)
    summed = pl.pallas_call(
        functools.partial(total_kernel, piece), out_shape=packed_type, in_specs=[vmem], out_specs=vmem, name="total"
    )(exchange(packed))
    everything = exchange(summed)
    square = (width, width)
    whitened, energy = pl.pallas_call(
        functools.partial(whiten_kernel, rows_total),
        out_shape=(jax.ShapeDtypeStruct((rows_dev, width), BF16), jax.ShapeDtypeStruct((1, 1), F32)),
        in_specs=[vmem, vmem],
        out_specs=(vmem, vmem),
        scratch_shapes=[pltpu.VMEM(square, F32)] * 3 + [pltpu.VMEM(square, BF16)] * 7,
        name="whiten",
    )(embeddings, everything)
    return whitened, energy.reshape(())


def solution(mesh):
    torus = Mesh(mesh.devices.reshape(mesh.shape["grp"], 8, 4, 2), AXES)
    return jax.shard_map(
        local, mesh=torus, in_specs=(P(AXES, None),), out_specs=(P(AXES, None), P()), check_vma=False
    )
```

```python
import functools

import jax
import jax.numpy as jnp
from jax import lax
from jax.experimental import pallas as pl
from jax.experimental.pallas import tpu as pltpu
from jax.sharding import Mesh
from jax.sharding import PartitionSpec as P

ITERS = 4
AXES = ("grp", "row_0", "row_1", "row_2")
LANES = 128
TILE = 256
F32 = jnp.float32
BF16 = jnp.bfloat16


def layout(width):
    nb = width // LANES
    place = {}
    at = [0, 0]
    for i in range(nb):
        half = 0 if i < TILE // LANES else 1
        for j in range(i, nb):
            if j == i and i % 2:
                continue
            place[i, j] = (half, at[half])
            at[half] += LANES
    return nb, place, at[1], max(at[0], at[1] + 16)


def upper(shape):
    r = lax.broadcasted_iota(jnp.int32, shape, 0)
    c = lax.broadcasted_iota(jnp.int32, shape, 1)
    return r <= c, r == c


def gram_kernel(e_ref, *refs):
    o_ref = refs[-1]
    width = e_ref.shape[1]
    nb, place, tail, _ = layout(width)
    core = lax.axis_index(AXES[3])

    def put(at, rows):
        if len(refs) > 1:
            rows = rows + refs[0][at : at + rows.shape[0], :]
        o_ref[at : at + rows.shape[0], :] = rows

    def tile_row(big):
        keep, _ = upper((LANES, LANES))
        g = lax.dot_general(
            e_ref[:, big : big + TILE], e_ref[:, big:], (((0,), (0,)), ((), ())), preferred_element_type=F32
        )
        i = big // LANES

        def block(r, j):
            return g[r * LANES : (r + 1) * LANES, j * LANES - big : (j + 1) * LANES - big]

        put(place[i, i][1], jnp.where(keep, block(0, i), block(1, i + 1)))
        for r in range(2):
            for j in range(i + r + 1, nb):
                put(place[i + r, j][1], block(r, j))

    @pl.when(core == 0)
    def _():
        tile_row(0)

    @pl.when(core == 1)
    def _():
        for big in range(TILE, width, TILE):
            tile_row(big)
        e = e_ref[...].astype(F32)
        colsum = jnp.sum(e, axis=0, keepdims=True)
        lines = [colsum[:, k * LANES : (k + 1) * LANES] for k in range(nb)]
        for k in range(1, nb, 2):
            x = e[:, k * LANES : (k + 1) * LANES]
            lines.append(jnp.sum(x * x, axis=0, keepdims=True))
        used = tail + len(lines)
        for k, line in enumerate(lines):
            put(tail + k, line)
        o_ref[used:, :] = jnp.zeros((o_ref.shape[0] - used, LANES), F32)


def total_kernel(piece, x_ref, o_ref):
    period = 8 * piece
    groups = x_ref.shape[0] // period
    acc = jnp.sum(x_ref[...].reshape(groups, period, LANES), axis=0)
    for shift in (piece, 2 * piece, 4 * piece):
        acc = acc + jnp.concatenate([acc[period - shift :], acc[: period - shift]], axis=0)
    for g in range(groups):
        o_ref[g * period : (g + 1) * period, :] = acc


def split(x):
    hi = x.astype(BF16)
    lo = (x - hi.astype(F32)).astype(BF16)
    return hi, lo


def whiten_kernel(rows_total, e_ref, own_ref, other_ref, o_ref, en_ref, half_ref, s_ref, r_ref, q_ref, sh, sl, ah, al, bh, bl, w_ref):
    rows_dev, width = e_ref.shape
    nb, place, tail, _ = layout(width)
    inv = 1.0 / rows_total
    keep, diag = upper((LANES, LANES))
    core = lax.axis_index(AXES[3])
    half_ref[core] = own_ref[...]
    half_ref[1 - core] = other_ref[...]

    def packed(i, j):
        half, at = place[i, j]
        return half_ref[half, at : at + LANES, :]

    def line(k):
        return half_ref[1, tail + k : tail + k + 1, :]

    means = [line(k) * inv for k in range(nb)]
    down = [jnp.transpose(jnp.broadcast_to(m, (LANES, LANES))) for m in means]

    squares = jnp.zeros((LANES, LANES), F32)
    for i in range(nb):
        for j in range(i, nb):
            if i != j:
                block = packed(i, j)
            else:
                base = i - i % 2
                both = packed(base, base)
                mirror = jnp.transpose(both)
                if i == base:
                    block = jnp.where(keep, both, mirror)
                else:
                    block = jnp.where(diag, line(nb + base // 2), jnp.where(keep, mirror, both))
            cov = block * inv - down[i] * means[j]
            squares = squares + (cov * cov) * (1.0 if i == j else 2.0)
            s_ref[i * LANES : (i + 1) * LANES, j * LANES : (j + 1) * LANES] = cov
    total = jnp.sum(jnp.sum(squares, axis=0, keepdims=True), axis=1, keepdims=True)
    fro = jnp.sqrt(total + 1e-06)
    rescale = 1.0 / fro
    for i in range(nb):
        for j in range(i, nb):
            at = (slice(i * LANES, (i + 1) * LANES), slice(j * LANES, (j + 1) * LANES))
            s = s_ref[at] * rescale
            s_ref[at] = s
            sh[at], sl[at] = split(s)
            if i != j:
                turned = jnp.transpose(s)
                ta = (at[1], at[0])
                sh[ta], sl[ta] = split(turned)
                if i // (TILE // LANES) == j // (TILE // LANES):
                    s_ref[ta] = turned

    nt = width // TILE
    pairs = [(i, j) for i in range(nt) for j in range(i, nt)]

    def span(i):
        return slice(i * TILE, (i + 1) * TILE)

    def dot(a, b):
        return jnp.dot(a, b, preferred_element_type=F32)

    def product(xh, xl, yh, yl, i, j):
        a, b = span(i), span(j)
        return dot(xh[a, :], yh[:, b]) + (dot(xh[a, :], yl[:, b]) + dot(xl[a, :], yh[:, b]))

    def put(h_ref, l_ref, i, j, x):
        h_ref[span(i), span(j)], l_ref[span(i), span(j)] = split(x)
        if i != j:
            h_ref[span(j), span(i)], l_ref[span(j), span(i)] = split(jnp.transpose(x))

    def double_step(t_ref, th, tl, x_ref):
        for i, j in pairs:
            at = (span(i), span(j))
            t2 = product(th, tl, th, tl, i, j)
            t = t_ref[at]
            put(ah, al, i, j, t2)
            put(bh, bl, i, j, 0.0625 * t2 - 0.5625 * t)
            x_ref[at] = 1.6875 * t2 - 2.4375 * t
        for i, j in pairs:
            at = (span(i), span(j))
            x_ref[at] = x_ref[at] + product(ah, al, bh, bl, i, j)

    double_step(s_ref, sh, sl, r_ref)
    for i, j in pairs:
        put(ah, al, i, j, r_ref[span(i), span(j)])
    for i, j in pairs:
        at = (span(i), span(j))
        put(bh, bl, i, j, 4.5 * r_ref[at] + product(ah, al, ah, al, i, j))
    for i, j in pairs:
        at = (span(i), span(j))
        q_ref[at] = 5.0625 * s_ref[at] + product(sh, sl, bh, bl, i, j)
    for i, j in pairs:
        put(sh, sl, i, j, q_ref[span(i), span(j)])
    double_step(q_ref, sh, sl, q_ref)
    for i, j in pairs:
        put(ah, al, i, j, r_ref[span(i), span(j)])
        put(bh, bl, i, j, q_ref[span(i), span(j)])
    root = lax.rsqrt(fro)
    one = upper((TILE, TILE))[1]
    for i, j in pairs:
        at = (span(i), span(j))
        z = 2.25 * (r_ref[at] + q_ref[at]) + product(ah, al, bh, bl, i, j)
        if i == j:
            z = z + jnp.where(one, 5.0625, 0.0)
        w = (z * root).astype(BF16)
        w_ref[at] = w
        if i != j:
            w_ref[span(j), span(i)] = jnp.transpose(w.astype(F32)).astype(BF16)

    acc = jnp.zeros((TILE, TILE), F32)
    for i, j in pairs:
        g = dot(w_ref[span(i), :], w_ref[:, span(j)])
        acc = acc + g * s_ref[span(i), span(j)] * (1.0 if i == j else 2.0)
    trace = jnp.sum(jnp.sum(acc, axis=0, keepdims=True), axis=1, keepdims=True)
    en_ref[...] = trace * fro * (1.0 / width)

    mean = jnp.concatenate(means, axis=1)
    for r in range(0, rows_dev, TILE):
        c = (e_ref[r : r + TILE, :].astype(F32) - mean).astype(BF16)
        o_ref[r : r + TILE, :] = dot(c, w_ref[...]).astype(BF16)


def local(embeddings):
    rows_dev, width = embeddings.shape
    rows_total = rows_dev * lax.axis_size(AXES)
    chips = lax.axis_size(AXES[:3])
    _, _, _, need = layout(width)
    piece = -(-need // chips)
    rows = piece * chips
    half_type = jax.ShapeDtypeStruct((rows, LANES), F32)
    vmem = pl.BlockSpec(memory_space=pltpu.VMEM)

    def exchange(x):
        x = x.reshape(chips, 1, piece * LANES)
        return lax.all_to_all(x, AXES[:3], 0, 0, tiled=True).reshape(rows, LANES)

    def swap(x):
        return lax.ppermute(x, AXES[3], [(0, 1), (1, 0)])

    def call(kernel, out, name, *args, flops=0, mib=8, **rest):
        cost = pl.CostEstimate(flops=flops, bytes_accessed=0, transcendentals=0)
        return pl.pallas_call(
            kernel,
            out_shape=out,
            in_specs=[vmem] * len(args),
            out_specs=jax.tree.map(lambda _: vmem, out),
            cost_estimate=cost,
            compiler_params=pltpu.CompilerParams(vmem_limit_bytes=mib << 20),
            name=name,
            **rest,
        )(*args)

    flops = 2 * rows_dev * width * TILE
    theirs = swap(embeddings)
    own = call(gram_kernel, half_type, "gram_own", embeddings, flops=flops)
    packed = call(gram_kernel, half_type, "gram_both", theirs, own, flops=flops)
    summed = call(functools.partial(total_kernel, piece), half_type, "total", exchange(packed))
    half = exchange(summed)
    square = (width, width)
    whitened, energy = call(
        functools.partial(whiten_kernel, rows_total),
        (jax.ShapeDtypeStruct((rows_dev, width), BF16), jax.ShapeDtypeStruct((1, 1), F32)),
        "whiten",
        embeddings,
        half,
        swap(half),
        flops=40 * width**3,
        mib=32,
        scratch_shapes=[pltpu.VMEM((2, rows, LANES), F32)]
        + [pltpu.VMEM(square, F32)] * 3
        + [pltpu.VMEM(square, BF16)] * 7,
    )
    return whitened, energy.reshape(())


def solution(mesh):
    torus = Mesh(mesh.devices.reshape(mesh.shape["grp"], 8, 4, 2), AXES)
    return jax.shard_map(
        local, mesh=torus, in_specs=(P(AXES, None),), out_specs=(P(AXES, None), P()), check_vma=False
    )
```

```python
import functools

import jax
import jax.numpy as jnp
from jax import lax
from jax.experimental import pallas as pl
from jax.experimental.pallas import tpu as pltpu
from jax.sharding import Mesh
from jax.sharding import PartitionSpec as P

ITERS = 4
AXES = ("grp", "row_0", "row_1", "row_2")
LANES = 128
TILE = 256
F32 = jnp.float32
BF16 = jnp.bfloat16


def layout(width):
    nb = width // LANES
    place = {}
    at = [0, 0]
    for i in range(nb):
        half = 0 if i < TILE // LANES else 1
        for j in range(i, nb):
            if j == i and i % 2:
                continue
            place[i, j] = (half, at[half])
            at[half] += LANES
    return nb, place, at[1], max(at[0], at[1] + 16)


def upper(shape):
    r = lax.broadcasted_iota(jnp.int32, shape, 0)
    c = lax.broadcasted_iota(jnp.int32, shape, 1)
    return r <= c, r == c


def gram_kernel(e_ref, *refs):
    o_ref = refs[-1]
    width = e_ref.shape[1]
    nb, place, tail, _ = layout(width)
    core = lax.axis_index(AXES[3])

    def put(at, rows):
        if len(refs) > 1:
            rows = rows + refs[0][at : at + rows.shape[0], :]
        o_ref[at : at + rows.shape[0], :] = rows

    def tile_row(big):
        keep, _ = upper((LANES, LANES))
        g = lax.dot_general(
            e_ref[:, big : big + TILE], e_ref[:, big:], (((0,), (0,)), ((), ())), preferred_element_type=F32
        )
        i = big // LANES

        def block(r, j):
            return g[r * LANES : (r + 1) * LANES, j * LANES - big : (j + 1) * LANES - big]

        put(place[i, i][1], jnp.where(keep, block(0, i), block(1, i + 1)))
        for r in range(2):
            for j in range(i + r + 1, nb):
                put(place[i + r, j][1], block(r, j))

    @pl.when(core == 0)
    def _():
        tile_row(0)

    @pl.when(core == 1)
    def _():
        for big in range(TILE, width, TILE):
            tile_row(big)
        e = e_ref[...].astype(F32)
        colsum = jnp.sum(e, axis=0, keepdims=True)
        lines = [colsum[:, k * LANES : (k + 1) * LANES] for k in range(nb)]
        for k in range(1, nb, 2):
            x = e[:, k * LANES : (k + 1) * LANES]
            lines.append(jnp.sum(x * x, axis=0, keepdims=True))
        used = tail + len(lines)
        for k, line in enumerate(lines):
            put(tail + k, line)
        o_ref[used:, :] = jnp.zeros((o_ref.shape[0] - used, LANES), F32)


def total_kernel(peers, copies, x_ref, o_ref):
    rows = x_ref.shape[0] // peers
    acc = x_ref[:rows, :]
    for n in range(1, peers):
        acc = acc + x_ref[n * rows : (n + 1) * rows, :]
    for n in range(copies):
        o_ref[n * rows : (n + 1) * rows, :] = acc


def split(x):
    hi = x.astype(BF16)
    lo = (x - hi.astype(F32)).astype(BF16)
    return hi, lo


def whiten_kernel(rows_total, e_ref, own_ref, other_ref, o_ref, en_ref, half_ref, s_ref, r_ref, q_ref, sh, sl, ah, al, bh, bl, w_ref):
    rows_dev, width = e_ref.shape
    nb, place, tail, _ = layout(width)
    inv = 1.0 / rows_total
    keep, diag = upper((LANES, LANES))
    core = lax.axis_index(AXES[3])
    half_ref[core] = own_ref[...]
    half_ref[1 - core] = other_ref[...]

    def packed(i, j):
        half, at = place[i, j]
        return half_ref[half, at : at + LANES, :]

    def line(k):
        return half_ref[1, tail + k : tail + k + 1, :]

    means = [line(k) * inv for k in range(nb)]
    down = [jnp.transpose(jnp.broadcast_to(m, (LANES, LANES))) for m in means]

    squares = jnp.zeros((LANES, LANES), F32)
    for i in range(nb):
        for j in range(i, nb):
            if i != j:
                block = packed(i, j)
            else:
                base = i - i % 2
                both = packed(base, base)
                mirror = jnp.transpose(both)
                if i == base:
                    block = jnp.where(keep, both, mirror)
                else:
                    block = jnp.where(diag, line(nb + base // 2), jnp.where(keep, mirror, both))
            cov = block * inv - down[i] * means[j]
            squares = squares + (cov * cov) * (1.0 if i == j else 2.0)
            s_ref[i * LANES : (i + 1) * LANES, j * LANES : (j + 1) * LANES] = cov
    total = jnp.sum(jnp.sum(squares, axis=0, keepdims=True), axis=1, keepdims=True)
    fro = jnp.sqrt(total + 1e-06)
    rescale = 1.0 / fro
    for i in range(nb):
        for j in range(i, nb):
            at = (slice(i * LANES, (i + 1) * LANES), slice(j * LANES, (j + 1) * LANES))
            s = s_ref[at] * rescale
            s_ref[at] = s
            sh[at], sl[at] = split(s)
            if i != j:
                turned = jnp.transpose(s)
                ta = (at[1], at[0])
                sh[ta], sl[ta] = split(turned)
                if i // (TILE // LANES) == j // (TILE // LANES):
                    s_ref[ta] = turned

    nt = width // TILE
    pairs = [(i, j) for i in range(nt) for j in range(i, nt)]

    def span(i):
        return slice(i * TILE, (i + 1) * TILE)

    def dot(a, b):
        return jnp.dot(a, b, preferred_element_type=F32)

    def product(xh, xl, yh, yl, i, j):
        a, b = span(i), span(j)
        return dot(xh[a, :], yh[:, b]) + (dot(xh[a, :], yl[:, b]) + dot(xl[a, :], yh[:, b]))

    def put(h_ref, l_ref, i, j, x):
        h_ref[span(i), span(j)], l_ref[span(i), span(j)] = split(x)
        if i != j:
            h_ref[span(j), span(i)], l_ref[span(j), span(i)] = split(jnp.transpose(x))

    def double_step(t_ref, th, tl, x_ref):
        for i, j in pairs:
            at = (span(i), span(j))
            t2 = product(th, tl, th, tl, i, j)
            t = t_ref[at]
            put(ah, al, i, j, t2)
            put(bh, bl, i, j, 0.0625 * t2 - 0.5625 * t)
            x_ref[at] = 1.6875 * t2 - 2.4375 * t
        for i, j in pairs:
            at = (span(i), span(j))
            x_ref[at] = x_ref[at] + product(ah, al, bh, bl, i, j)

    double_step(s_ref, sh, sl, r_ref)
    for i, j in pairs:
        put(ah, al, i, j, r_ref[span(i), span(j)])
    for i, j in pairs:
        at = (span(i), span(j))
        put(bh, bl, i, j, 4.5 * r_ref[at] + product(ah, al, ah, al, i, j))
    for i, j in pairs:
        at = (span(i), span(j))
        q_ref[at] = 5.0625 * s_ref[at] + product(sh, sl, bh, bl, i, j)
    for i, j in pairs:
        put(sh, sl, i, j, q_ref[span(i), span(j)])
    double_step(q_ref, sh, sl, q_ref)
    for i, j in pairs:
        put(ah, al, i, j, r_ref[span(i), span(j)])
        put(bh, bl, i, j, q_ref[span(i), span(j)])
    root = lax.rsqrt(fro)
    one = upper((TILE, TILE))[1]
    for i, j in pairs:
        at = (span(i), span(j))
        z = 2.25 * (r_ref[at] + q_ref[at]) + product(ah, al, bh, bl, i, j)
        if i == j:
            z = z + jnp.where(one, 5.0625, 0.0)
        w = (z * root).astype(BF16)
        w_ref[at] = w
        if i != j:
            w_ref[span(j), span(i)] = jnp.transpose(w.astype(F32)).astype(BF16)

    acc = jnp.zeros((TILE, TILE), F32)
    for i, j in pairs:
        g = dot(w_ref[span(i), :], w_ref[:, span(j)])
        acc = acc + g * s_ref[span(i), span(j)] * (1.0 if i == j else 2.0)
    trace = jnp.sum(jnp.sum(acc, axis=0, keepdims=True), axis=1, keepdims=True)
    en_ref[...] = trace * fro * (1.0 / width)

    mean = jnp.concatenate(means, axis=1)
    for r in range(0, rows_dev, TILE):
        c = (e_ref[r : r + TILE, :].astype(F32) - mean).astype(BF16)
        o_ref[r : r + TILE, :] = dot(c, w_ref[...]).astype(BF16)


def local(embeddings):
    rows_dev, width = embeddings.shape
    rows_total = rows_dev * lax.axis_size(AXES)
    sizes = [lax.axis_size(axis) for axis in AXES]
    _, _, _, need = layout(width)
    unit = 8 * sizes[0] * sizes[2]
    rows = -(-need // unit) * unit
    half_type = jax.ShapeDtypeStruct((rows, LANES), F32)
    vmem = pl.BlockSpec(memory_space=pltpu.VMEM)

    def exchange(x, n):
        y = x.reshape(sizes[n], 1, x.shape[0] * LANES // sizes[n])
        return lax.all_to_all(y, AXES[n], 0, 0, tiled=True).reshape(x.shape)

    def swap(x):
        return lax.ppermute(x, AXES[3], [(0, 1), (1, 0)])

    def call(kernel, out, name, *args, flops=0, mib=8, **rest):
        cost = pl.CostEstimate(flops=flops, bytes_accessed=0, transcendentals=0)
        return pl.pallas_call(
            kernel,
            out_shape=out,
            in_specs=[vmem] * len(args),
            out_specs=jax.tree.map(lambda _: vmem, out),
            cost_estimate=cost,
            compiler_params=pltpu.CompilerParams(vmem_limit_bytes=mib << 20),
            name=name,
            **rest,
        )(*args)

    flops = 2 * rows_dev * width * TILE
    theirs = swap(embeddings)
    own = call(gram_kernel, half_type, "gram_own", embeddings, flops=flops)
    packed = call(gram_kernel, half_type, "gram_both", theirs, own, flops=flops)

    def total(x, peers, copies):
        out = jax.ShapeDtypeStruct((x.shape[0] // peers * copies, LANES), F32)
        return call(functools.partial(total_kernel, peers, copies), out, f"total_{peers}_{copies}", x)

    x = total(exchange(packed, 2), sizes[2], 1)
    x = total(exchange(x, 0), sizes[0], sizes[1])
    x = total(exchange(x, 1), sizes[1], sizes[0])
    x = total(exchange(x, 0), 1, sizes[2])
    half = exchange(x, 2)
    square = (width, width)
    whitened, energy = call(
        functools.partial(whiten_kernel, rows_total),
        (jax.ShapeDtypeStruct((rows_dev, width), BF16), jax.ShapeDtypeStruct((1, 1), F32)),
        "whiten",
        embeddings,
        half,
        swap(half),
        flops=40 * width**3,
        mib=32,
        scratch_shapes=[pltpu.VMEM((2, rows, LANES), F32)]
        + [pltpu.VMEM(square, F32)] * 3
        + [pltpu.VMEM(square, BF16)] * 7,
    )
    return whitened, energy.reshape(())


def solution(mesh):
    torus = Mesh(mesh.devices.reshape(mesh.shape["grp"], 8, 4, 2), AXES)
    return jax.shard_map(
        local, mesh=torus, in_specs=(P(AXES, None),), out_specs=(P(AXES, None), P()), check_vma=False
    )
```

```python
import functools

import jax
import jax.numpy as jnp
from jax import lax
from jax.experimental import pallas as pl
from jax.experimental.pallas import tpu as pltpu
from jax.sharding import Mesh
from jax.sharding import PartitionSpec as P

ITERS = 4
AXES = ("grp", "row_0", "row_1", "row_2")
PLANE = ("grp", "row_1")
LANES = 128
TILE = 256
F32 = jnp.float32
BF16 = jnp.bfloat16


def layout(width):
    nb = width // LANES
    place = {}
    at = [0, 0]
    for i in range(nb):
        half = 0 if i < TILE // LANES else 1
        for j in range(i, nb):
            if j == i and i % 2:
                continue
            place[i, j] = (half, at[half])
            at[half] += LANES
    return nb, place, at[1], max(at[0], at[1] + 16)


def upper(shape):
    r = lax.broadcasted_iota(jnp.int32, shape, 0)
    c = lax.broadcasted_iota(jnp.int32, shape, 1)
    return r <= c, r == c


def gram_kernel(e_ref, *refs):
    o_ref = refs[-1]
    width = e_ref.shape[1]
    nb, place, tail, _ = layout(width)
    core = lax.axis_index(AXES[3])

    def put(at, rows):
        if len(refs) > 1:
            rows = rows + refs[0][at : at + rows.shape[0], :]
        o_ref[at : at + rows.shape[0], :] = rows

    def tile_row(big):
        keep, _ = upper((LANES, LANES))
        g = lax.dot_general(
            e_ref[:, big : big + TILE], e_ref[:, big:], (((0,), (0,)), ((), ())), preferred_element_type=F32
        )
        i = big // LANES

        def block(r, j):
            return g[r * LANES : (r + 1) * LANES, j * LANES - big : (j + 1) * LANES - big]

        put(place[i, i][1], jnp.where(keep, block(0, i), block(1, i + 1)))
        for r in range(2):
            for j in range(i + r + 1, nb):
                put(place[i + r, j][1], block(r, j))

    @pl.when(core == 0)
    def _():
        tile_row(0)

    @pl.when(core == 1)
    def _():
        for big in range(TILE, width, TILE):
            tile_row(big)
        e = e_ref[...].astype(F32)
        colsum = jnp.sum(e, axis=0, keepdims=True)
        lines = [colsum[:, k * LANES : (k + 1) * LANES] for k in range(nb)]
        for k in range(1, nb, 2):
            x = e[:, k * LANES : (k + 1) * LANES]
            lines.append(jnp.sum(x * x, axis=0, keepdims=True))
        used = tail + len(lines)
        for k, line in enumerate(lines):
            put(tail + k, line)
        o_ref[used:, :] = jnp.zeros((o_ref.shape[0] - used, LANES), F32)


def total_kernel(peers, copies, x_ref, o_ref):
    rows = x_ref.shape[0] // peers
    acc = x_ref[:rows, :]
    for n in range(1, peers):
        acc = acc + x_ref[n * rows : (n + 1) * rows, :]
    for n in range(copies):
        o_ref[n * rows : (n + 1) * rows, :] = acc


def split(x):
    hi = x.astype(BF16)
    lo = (x - hi.astype(F32)).astype(BF16)
    return hi, lo


def whiten_kernel(rows_total, e_ref, own_ref, other_ref, o_ref, en_ref, half_ref, s_ref, r_ref, q_ref, sh, sl, ah, al, bh, bl, w_ref):
    rows_dev, width = e_ref.shape
    nb, place, tail, _ = layout(width)
    inv = 1.0 / rows_total
    keep, diag = upper((LANES, LANES))
    core = lax.axis_index(AXES[3])
    half_ref[core] = own_ref[...]
    half_ref[1 - core] = other_ref[...]

    def packed(i, j):
        half, at = place[i, j]
        return half_ref[half, at : at + LANES, :]

    def line(k):
        return half_ref[1, tail + k : tail + k + 1, :]

    means = [line(k) * inv for k in range(nb)]
    down = [jnp.transpose(jnp.broadcast_to(m, (LANES, LANES))) for m in means]

    squares = jnp.zeros((LANES, LANES), F32)
    for i in range(nb):
        for j in range(i, nb):
            if i != j:
                block = packed(i, j)
            else:
                base = i - i % 2
                both = packed(base, base)
                mirror = jnp.transpose(both)
                if i == base:
                    block = jnp.where(keep, both, mirror)
                else:
                    block = jnp.where(diag, line(nb + base // 2), jnp.where(keep, mirror, both))
            cov = block * inv - down[i] * means[j]
            squares = squares + (cov * cov) * (1.0 if i == j else 2.0)
            s_ref[i * LANES : (i + 1) * LANES, j * LANES : (j + 1) * LANES] = cov
    total = jnp.sum(jnp.sum(squares, axis=0, keepdims=True), axis=1, keepdims=True)
    fro = jnp.sqrt(total + 1e-06)
    rescale = 1.0 / fro
    for i in range(nb):
        for j in range(i, nb):
            at = (slice(i * LANES, (i + 1) * LANES), slice(j * LANES, (j + 1) * LANES))
            s = s_ref[at] * rescale
            s_ref[at] = s
            sh[at], sl[at] = split(s)
            if i != j:
                turned = jnp.transpose(s)
                ta = (at[1], at[0])
                sh[ta], sl[ta] = split(turned)
                if i // (TILE // LANES) == j // (TILE // LANES):
                    s_ref[ta] = turned

    nt = width // TILE
    pairs = [(i, j) for i in range(nt) for j in range(i, nt)]

    def span(i):
        return slice(i * TILE, (i + 1) * TILE)

    def dot(a, b):
        return jnp.dot(a, b, preferred_element_type=F32)

    def product(xh, xl, yh, yl, i, j):
        a, b = span(i), span(j)
        return dot(xh[a, :], yh[:, b]) + (dot(xh[a, :], yl[:, b]) + dot(xl[a, :], yh[:, b]))

    def squared(xh, xl, i, j):
        if i != j:
            return product(xh, xl, xh, xl, i, j)
        a = span(i)
        cross = dot(xh[a, :], xl[:, a])
        return dot(xh[a, :], xh[:, a]) + (cross + jnp.transpose(cross))

    def put(h_ref, l_ref, i, j, x):
        h_ref[span(i), span(j)], l_ref[span(i), span(j)] = split(x)
        if i != j:
            h_ref[span(j), span(i)], l_ref[span(j), span(i)] = split(jnp.transpose(x))

    def double_step(t_ref, th, tl, x_ref):
        for i, j in pairs:
            at = (span(i), span(j))
            t2 = squared(th, tl, i, j)
            t = t_ref[at]
            put(ah, al, i, j, t2)
            put(bh, bl, i, j, 0.0625 * t2 - 0.5625 * t)
            x_ref[at] = 1.6875 * t2 - 2.4375 * t
        for i, j in pairs:
            at = (span(i), span(j))
            x_ref[at] = x_ref[at] + product(ah, al, bh, bl, i, j)

    double_step(s_ref, sh, sl, r_ref)
    for i, j in pairs:
        put(ah, al, i, j, r_ref[span(i), span(j)])
    for i, j in pairs:
        at = (span(i), span(j))
        put(bh, bl, i, j, 4.5 * r_ref[at] + squared(ah, al, i, j))
    for i, j in pairs:
        at = (span(i), span(j))
        q_ref[at] = 5.0625 * s_ref[at] + product(sh, sl, bh, bl, i, j)
    for i, j in pairs:
        put(sh, sl, i, j, q_ref[span(i), span(j)])
    double_step(q_ref, sh, sl, q_ref)
    for i, j in pairs:
        put(ah, al, i, j, r_ref[span(i), span(j)])
        put(bh, bl, i, j, q_ref[span(i), span(j)])
    root = lax.rsqrt(fro)
    one = upper((TILE, TILE))[1]
    for i, j in pairs:
        at = (span(i), span(j))
        z = 2.25 * (r_ref[at] + q_ref[at]) + product(ah, al, bh, bl, i, j)
        if i == j:
            z = z + jnp.where(one, 5.0625, 0.0)
        w = (z * root).astype(BF16)
        w_ref[at] = w
        if i != j:
            w_ref[span(j), span(i)] = jnp.transpose(w.astype(F32)).astype(BF16)

    acc = jnp.zeros((TILE, TILE), F32)
    for i, j in pairs:
        g = dot(w_ref[span(i), :], w_ref[:, span(j)])
        acc = acc + g * s_ref[span(i), span(j)] * (1.0 if i == j else 2.0)
    trace = jnp.sum(jnp.sum(acc, axis=0, keepdims=True), axis=1, keepdims=True)
    en_ref[...] = trace * fro * (1.0 / width)

    mean = jnp.concatenate(means, axis=1)
    for r in range(0, rows_dev, TILE):
        c = (e_ref[r : r + TILE, :].astype(F32) - mean).astype(BF16)
        o_ref[r : r + TILE, :] = dot(c, w_ref[...]).astype(BF16)


def local(embeddings):
    rows_dev, width = embeddings.shape
    rows_total = rows_dev * lax.axis_size(AXES)
    sizes = [lax.axis_size(axis) for axis in AXES]
    _, _, _, need = layout(width)
    plane = lax.axis_size(PLANE)
    unit = 8 * plane
    rows = -(-need // unit) * unit
    half_type = jax.ShapeDtypeStruct((rows, LANES), F32)
    vmem = pl.BlockSpec(memory_space=pltpu.VMEM)

    def exchange(x, axes):
        peers = lax.axis_size(axes)
        y = x.reshape(peers, 1, x.shape[0] * LANES // peers)
        return lax.all_to_all(y, axes, 0, 0, tiled=True).reshape(x.shape)

    def swap(x):
        return lax.ppermute(x, AXES[3], [(0, 1), (1, 0)])

    def call(kernel, out, name, *args, flops=0, mib=8, **rest):
        cost = pl.CostEstimate(flops=flops, bytes_accessed=0, transcendentals=0)
        return pl.pallas_call(
            kernel,
            out_shape=out,
            in_specs=[vmem] * len(args),
            out_specs=jax.tree.map(lambda _: vmem, out),
            cost_estimate=cost,
            compiler_params=pltpu.CompilerParams(vmem_limit_bytes=mib << 20),
            name=name,
            **rest,
        )(*args)

    flops = 2 * rows_dev * width * TILE
    theirs = swap(embeddings)
    own = call(gram_kernel, half_type, "gram_own", embeddings, flops=flops)
    packed = call(gram_kernel, half_type, "gram_both", theirs, own, flops=flops)

    def total(x, peers, copies):
        out = jax.ShapeDtypeStruct((x.shape[0] // peers * copies, LANES), F32)
        return call(functools.partial(total_kernel, peers, copies), out, f"total_{peers}_{copies}", x)

    x = total(exchange(packed, PLANE), plane, sizes[1])
    x = total(exchange(x, AXES[1]), sizes[1], plane)
    half = exchange(x, PLANE)
    square = (width, width)
    whitened, energy = call(
        functools.partial(whiten_kernel, rows_total),
        (jax.ShapeDtypeStruct((rows_dev, width), BF16), jax.ShapeDtypeStruct((1, 1), F32)),
        "whiten",
        embeddings,
        half,
        swap(half),
        flops=40 * width**3,
        mib=32,
        scratch_shapes=[pltpu.VMEM((2, rows, LANES), F32)]
        + [pltpu.VMEM(square, F32)] * 3
        + [pltpu.VMEM(square, BF16)] * 7,
    )
    return whitened, energy.reshape(())


def solution(mesh):
    torus = Mesh(mesh.devices.reshape(mesh.shape["grp"], 8, 4, 2), AXES)
    return jax.shard_map(
        local, mesh=torus, in_specs=(P(AXES, None),), out_specs=(P(AXES, None), P()), check_vma=False
    )
```

```python
import functools

import jax
import jax.numpy as jnp
from jax import lax
from jax.experimental import pallas as pl
from jax.experimental.pallas import tpu as pltpu
from jax.sharding import Mesh
from jax.sharding import PartitionSpec as P

ITERS = 4
AXES = ("grp", "row_0", "row_1", "row_2")
LANES = 128
TILE = 256
F32 = jnp.float32
BF16 = jnp.bfloat16


def layout(width):
    nb = width // LANES
    place = {}
    at = [0, 0]
    for i in range(nb):
        half = 0 if i < TILE // LANES else 1
        for j in range(i, nb):
            if j == i and i % 2:
                continue
            place[i, j] = (half, at[half])
            at[half] += LANES
    return nb, place, at[1], max(at[0], at[1] + 16)


def upper(shape):
    r = lax.broadcasted_iota(jnp.int32, shape, 0)
    c = lax.broadcasted_iota(jnp.int32, shape, 1)
    return r <= c, r == c


def gram_kernel(e_ref, *refs):
    o_ref = refs[-1]
    width = e_ref.shape[1]
    nb, place, tail, _ = layout(width)
    core = lax.axis_index(AXES[3])

    def put(at, rows):
        if len(refs) > 1:
            rows = rows + refs[0][at : at + rows.shape[0], :]
        o_ref[at : at + rows.shape[0], :] = rows

    def tile_row(big):
        keep, _ = upper((LANES, LANES))
        g = lax.dot_general(
            e_ref[:, big : big + TILE], e_ref[:, big:], (((0,), (0,)), ((), ())), preferred_element_type=F32
        )
        i = big // LANES

        def block(r, j):
            return g[r * LANES : (r + 1) * LANES, j * LANES - big : (j + 1) * LANES - big]

        put(place[i, i][1], jnp.where(keep, block(0, i), block(1, i + 1)))
        for r in range(2):
            for j in range(i + r + 1, nb):
                put(place[i + r, j][1], block(r, j))

    @pl.when(core == 0)
    def _():
        tile_row(0)

    @pl.when(core == 1)
    def _():
        for big in range(TILE, width, TILE):
            tile_row(big)
        e = e_ref[...].astype(F32)
        colsum = jnp.sum(e, axis=0, keepdims=True)
        lines = [colsum[:, k * LANES : (k + 1) * LANES] for k in range(nb)]
        for k in range(1, nb, 2):
            x = e[:, k * LANES : (k + 1) * LANES]
            lines.append(jnp.sum(x * x, axis=0, keepdims=True))
        used = tail + len(lines)
        for k, line in enumerate(lines):
            put(tail + k, line)
        o_ref[used:, :] = jnp.zeros((o_ref.shape[0] - used, LANES), F32)


def total_kernel(peers, copies, x_ref, o_ref):
    rows = x_ref.shape[0] // peers
    acc = x_ref[:rows, :]
    for n in range(1, peers):
        acc = acc + x_ref[n * rows : (n + 1) * rows, :]
    for n in range(copies):
        o_ref[n * rows : (n + 1) * rows, :] = acc


def split(x):
    hi = x.astype(BF16)
    lo = (x - hi.astype(F32)).astype(BF16)
    return hi, lo


def whiten_kernel(rows_total, e_ref, own_ref, other_ref, o_ref, en_ref, half_ref, s_ref, r_ref, q_ref, sh, sl, ah, al, bh, bl, w_ref):
    rows_dev, width = e_ref.shape
    nb, place, tail, _ = layout(width)
    inv = 1.0 / rows_total
    keep, diag = upper((LANES, LANES))
    core = lax.axis_index(AXES[3])
    half_ref[core] = own_ref[...]
    half_ref[1 - core] = other_ref[...]

    def packed(i, j):
        half, at = place[i, j]
        return half_ref[half, at : at + LANES, :]

    def line(k):
        return half_ref[1, tail + k : tail + k + 1, :]

    means = [line(k) * inv for k in range(nb)]
    down = [jnp.transpose(jnp.broadcast_to(m, (LANES, LANES))) for m in means]

    squares = jnp.zeros((LANES, LANES), F32)
    for i in range(nb):
        for j in range(i, nb):
            if i != j:
                block = packed(i, j)
            else:
                base = i - i % 2
                both = packed(base, base)
                mirror = jnp.transpose(both)
                if i == base:
                    block = jnp.where(keep, both, mirror)
                else:
                    block = jnp.where(diag, line(nb + base // 2), jnp.where(keep, mirror, both))
            cov = block * inv - down[i] * means[j]
            squares = squares + (cov * cov) * (1.0 if i == j else 2.0)
            s_ref[i * LANES : (i + 1) * LANES, j * LANES : (j + 1) * LANES] = cov
    total = jnp.sum(jnp.sum(squares, axis=0, keepdims=True), axis=1, keepdims=True)
    fro = jnp.sqrt(total + 1e-06)
    rescale = 1.0 / fro
    for i in range(nb):
        for j in range(i, nb):
            at = (slice(i * LANES, (i + 1) * LANES), slice(j * LANES, (j + 1) * LANES))
            s = s_ref[at] * rescale
            s_ref[at] = s
            sh[at], sl[at] = split(s)
            if i != j:
                turned = jnp.transpose(s)
                ta = (at[1], at[0])
                sh[ta], sl[ta] = split(turned)
                if i // (TILE // LANES) == j // (TILE // LANES):
                    s_ref[ta] = turned

    nt = width // TILE
    pairs = [(i, j) for i in range(nt) for j in range(i, nt)]

    def span(i):
        return slice(i * TILE, (i + 1) * TILE)

    def dot(a, b):
        return jnp.dot(a, b, preferred_element_type=F32)

    def product(xh, xl, yh, yl, i, j):
        a, b = span(i), span(j)
        return dot(xh[a, :], yh[:, b]) + (dot(xh[a, :], yl[:, b]) + dot(xl[a, :], yh[:, b]))

    def squared(xh, xl, i, j):
        if i != j:
            return product(xh, xl, xh, xl, i, j)
        a = span(i)
        cross = dot(xh[a, :], xl[:, a])
        return dot(xh[a, :], xh[:, a]) + (cross + jnp.transpose(cross))

    def put(h_ref, l_ref, i, j, x):
        h_ref[span(i), span(j)], l_ref[span(i), span(j)] = split(x)
        if i != j:
            h_ref[span(j), span(i)], l_ref[span(j), span(i)] = split(jnp.transpose(x))

    def double_step(t_ref, th, tl, x_ref):
        for i, j in pairs:
            at = (span(i), span(j))
            t2 = squared(th, tl, i, j)
            t = t_ref[at]
            put(ah, al, i, j, t2)
            put(bh, bl, i, j, 0.0625 * t2 - 0.5625 * t)
            x_ref[at] = 1.6875 * t2 - 2.4375 * t
        for i, j in pairs:
            at = (span(i), span(j))
            x_ref[at] = x_ref[at] + product(ah, al, bh, bl, i, j)

    double_step(s_ref, sh, sl, r_ref)
    for i, j in pairs:
        put(ah, al, i, j, r_ref[span(i), span(j)])
    for i, j in pairs:
        at = (span(i), span(j))
        put(bh, bl, i, j, 4.5 * r_ref[at] + squared(ah, al, i, j))
    for i, j in pairs:
        at = (span(i), span(j))
        q_ref[at] = 5.0625 * s_ref[at] + product(sh, sl, bh, bl, i, j)
    for i, j in pairs:
        put(sh, sl, i, j, q_ref[span(i), span(j)])
    double_step(q_ref, sh, sl, q_ref)
    for i, j in pairs:
        put(ah, al, i, j, r_ref[span(i), span(j)])
        put(bh, bl, i, j, q_ref[span(i), span(j)])
    root = lax.rsqrt(fro)
    one = upper((TILE, TILE))[1]
    for i, j in pairs:
        at = (span(i), span(j))
        z = 2.25 * (r_ref[at] + q_ref[at]) + product(ah, al, bh, bl, i, j)
        if i == j:
            z = z + jnp.where(one, 5.0625, 0.0)
        w = (z * root).astype(BF16)
        w_ref[at] = w
        if i != j:
            w_ref[span(j), span(i)] = jnp.transpose(w.astype(F32)).astype(BF16)

    acc = jnp.zeros((TILE, TILE), F32)
    for i, j in pairs:
        g = dot(w_ref[span(i), :], w_ref[:, span(j)])
        acc = acc + g * s_ref[span(i), span(j)] * (1.0 if i == j else 2.0)
    trace = jnp.sum(jnp.sum(acc, axis=0, keepdims=True), axis=1, keepdims=True)
    en_ref[...] = trace * fro * (1.0 / width)

    mean = jnp.concatenate(means, axis=1)
    for r in range(0, rows_dev, TILE):
        c = (e_ref[r : r + TILE, :].astype(F32) - mean).astype(BF16)
        o_ref[r : r + TILE, :] = dot(c, w_ref[...]).astype(BF16)


def groups(sizes):
    ny, nz, nx, _ = sizes

    def at(y, z, x, core):
        return ((y * nz + z) * nx + x) * 2 + core

    planes = [[at(y, z, x, 0) for y in range(ny) for x in range(nx)] for z in range(nz)]
    planes += [[at(y, z, x, 1) for z in range(nz) for x in range(nx)] for y in range(ny)]
    lines = [[at(y, z, x, 0) for z in range(nz)] for y in range(ny) for x in range(nx)]
    lines += [[at(y, z, x, 1) for y in range(ny)] for z in range(nz) for x in range(nx)]
    return planes, lines


def local(embeddings):
    rows_dev, width = embeddings.shape
    rows_total = rows_dev * lax.axis_size(AXES)
    sizes = [lax.axis_size(axis) for axis in AXES]
    _, _, _, need = layout(width)
    vmem = pl.BlockSpec(memory_space=pltpu.VMEM)

    planes, lines = groups(sizes)
    plane, line = len(planes[0]), len(lines[0])
    rows = -(-need // (8 * plane)) * 8 * plane
    half_type = jax.ShapeDtypeStruct((rows, LANES), F32)

    def exchange(x, members):
        peers = len(members[0])
        y = x.reshape(peers, 1, x.shape[0] * LANES // peers)
        out = lax.all_to_all(y, AXES, 0, 0, axis_index_groups=members, tiled=True)
        return out.reshape(x.shape)

    def swap(x):
        return lax.ppermute(x, AXES[3], [(0, 1), (1, 0)])

    def call(kernel, out, name, *args, flops=0, mib=8, **rest):
        cost = pl.CostEstimate(flops=flops, bytes_accessed=0, transcendentals=0)
        return pl.pallas_call(
            kernel,
            out_shape=out,
            in_specs=[vmem] * len(args),
            out_specs=jax.tree.map(lambda _: vmem, out),
            cost_estimate=cost,
            compiler_params=pltpu.CompilerParams(vmem_limit_bytes=mib << 20),
            name=name,
            **rest,
        )(*args)

    flops = 2 * rows_dev * width * TILE
    theirs = swap(embeddings)
    own = call(gram_kernel, half_type, "gram_own", embeddings, flops=flops)
    packed = call(gram_kernel, half_type, "gram_both", theirs, own, flops=flops)

    def total(x, peers, copies):
        out = jax.ShapeDtypeStruct((x.shape[0] // peers * copies, LANES), F32)
        return call(functools.partial(total_kernel, peers, copies), out, f"total_{peers}_{copies}", x)

    x = total(exchange(packed, planes), plane, line)
    x = total(exchange(x, lines), line, plane)
    half = exchange(x, planes)
    square = (width, width)
    whitened, energy = call(
        functools.partial(whiten_kernel, rows_total),
        (jax.ShapeDtypeStruct((rows_dev, width), BF16), jax.ShapeDtypeStruct((1, 1), F32)),
        "whiten",
        embeddings,
        half,
        swap(half),
        flops=40 * width**3,
        mib=32,
        scratch_shapes=[pltpu.VMEM((2, rows, LANES), F32)]
        + [pltpu.VMEM(square, F32)] * 3
        + [pltpu.VMEM(square, BF16)] * 7,
    )
    return whitened, energy.reshape(())


def solution(mesh):
    torus = Mesh(mesh.devices.reshape(mesh.shape["grp"], 8, 4, 2), AXES)
    return jax.shard_map(
        local, mesh=torus, in_specs=(P(AXES, None),), out_specs=(P(AXES, None), P()), check_vma=False
    )
```

```python
import functools

import jax
import jax.numpy as jnp
from jax import lax
from jax.experimental import pallas as pl
from jax.experimental.pallas import tpu as pltpu
from jax.sharding import Mesh
from jax.sharding import PartitionSpec as P

ITERS = 4
AXES = ("grp", "row_0", "row_1", "row_2")
LANES = 128
TILE = 256
F32 = jnp.float32
BF16 = jnp.bfloat16


def layout(width):
    nb = width // LANES
    place = {}
    at = [0, 0]
    for i in range(nb):
        for j in range(i, nb):
            if j == i and i % 2:
                continue
            half = 0 if i < TILE // LANES and (i, j) != (1, nb - 1) else 1
            place[i, j] = (half, at[half])
            at[half] += LANES
    return nb, place, at[1], max(at[0], at[1] + nb + nb // 2)


def upper(shape):
    r = lax.broadcasted_iota(jnp.int32, shape, 0)
    c = lax.broadcasted_iota(jnp.int32, shape, 1)
    return r <= c, r == c


def gram_kernel(e_ref, *refs):
    o_ref = refs[-1]
    width = e_ref.shape[1]
    nb, place, tail, _ = layout(width)
    core = lax.axis_index(AXES[3])

    def put(at, rows):
        if len(refs) > 1:
            rows = rows + refs[0][at : at + rows.shape[0], :]
        o_ref[at : at + rows.shape[0], :] = rows

    def tile_row(big):
        keep, _ = upper((LANES, LANES))
        g = lax.dot_general(
            e_ref[:, big : big + TILE], e_ref[:, big:], (((0,), (0,)), ((), ())), preferred_element_type=F32
        )
        i = big // LANES

        def block(r, j):
            return g[r * LANES : (r + 1) * LANES, j * LANES - big : (j + 1) * LANES - big]

        put(place[i, i][1], jnp.where(keep, block(0, i), block(1, i + 1)))
        for r in range(2):
            for j in range(i + r + 1, nb):
                if (i + r, j) != (1, nb - 1):
                    put(place[i + r, j][1], block(r, j))

    @pl.when(core == 0)
    def _():
        tile_row(0)

    @pl.when(core == 1)
    def _():
        for big in range(TILE, width, TILE):
            tile_row(big)
        moved = lax.dot_general(
            e_ref[:, LANES:TILE], e_ref[:, width - LANES :], (((0,), (0,)), ((), ())), preferred_element_type=F32
        )
        put(place[1, nb - 1][1], moved)
        e = e_ref[...].astype(F32)
        colsum = jnp.sum(e, axis=0, keepdims=True)
        lines = [colsum[:, k * LANES : (k + 1) * LANES] for k in range(nb)]
        for k in range(1, nb, 2):
            x = e[:, k * LANES : (k + 1) * LANES]
            lines.append(jnp.sum(x * x, axis=0, keepdims=True))
        used = tail + len(lines)
        for k, line in enumerate(lines):
            put(tail + k, line)
        o_ref[used:, :] = jnp.zeros((o_ref.shape[0] - used, LANES), F32)


def total_kernel(peers, copies, x_ref, o_ref):
    rows = x_ref.shape[0] // peers
    acc = x_ref[:rows, :]
    for n in range(1, peers):
        acc = acc + x_ref[n * rows : (n + 1) * rows, :]
    for n in range(copies):
        o_ref[n * rows : (n + 1) * rows, :] = acc


def split(x):
    hi = x.astype(BF16)
    lo = (x - hi.astype(F32)).astype(BF16)
    return hi, lo


def whiten_kernel(rows_total, e_ref, own_ref, other_ref, o_ref, en_ref, half_ref, s_ref, r_ref, q_ref, sh, sl, ah, al, bh, bl, w_ref):
    rows_dev, width = e_ref.shape
    nb, place, tail, _ = layout(width)
    inv = 1.0 / rows_total
    keep, diag = upper((LANES, LANES))
    core = lax.axis_index(AXES[3])
    half_ref[core] = own_ref[...]
    half_ref[1 - core] = other_ref[...]

    def packed(i, j):
        half, at = place[i, j]
        return half_ref[half, at : at + LANES, :]

    def line(k):
        return half_ref[1, tail + k : tail + k + 1, :]

    means = [line(k) * inv for k in range(nb)]
    down = [jnp.transpose(jnp.broadcast_to(m, (LANES, LANES))) for m in means]

    squares = jnp.zeros((LANES, LANES), F32)
    for i in range(nb):
        for j in range(i, nb):
            if i != j:
                block = packed(i, j)
            else:
                base = i - i % 2
                both = packed(base, base)
                mirror = jnp.transpose(both)
                if i == base:
                    block = jnp.where(keep, both, mirror)
                else:
                    block = jnp.where(diag, line(nb + base // 2), jnp.where(keep, mirror, both))
            cov = block * inv - down[i] * means[j]
            squares = squares + (cov * cov) * (1.0 if i == j else 2.0)
            at = (slice(i * LANES, (i + 1) * LANES), slice(j * LANES, (j + 1) * LANES))
            s_ref[at] = cov
            sh[at], sl[at] = split(cov)
            if i != j:
                turned = jnp.transpose(cov)
                ta = (at[1], at[0])
                sh[ta], sl[ta] = split(turned)
                if i // (TILE // LANES) == j // (TILE // LANES):
                    s_ref[ta] = turned
    total = jnp.sum(jnp.sum(squares, axis=0, keepdims=True), axis=1, keepdims=True)
    fro = jnp.sqrt(total + 1e-06)
    rescale = 1.0 / fro

    nt = width // TILE
    pairs = [(i, j) for i in range(nt) for j in range(i, nt)]

    def span(i):
        return slice(i * TILE, (i + 1) * TILE)

    def dot(a, b):
        return jnp.dot(a, b, preferred_element_type=F32)

    def product(xh, xl, yh, yl, i, j):
        a, b = span(i), span(j)
        return dot(xh[a, :], yh[:, b]) + (dot(xh[a, :], yl[:, b]) + dot(xl[a, :], yh[:, b]))

    def squared(xh, xl, i, j):
        if i != j:
            return product(xh, xl, xh, xl, i, j)
        a = span(i)
        cross = dot(xh[a, :], xl[:, a])
        return dot(xh[a, :], xh[:, a]) + (cross + jnp.transpose(cross))

    def put(h_ref, l_ref, i, j, x):
        h_ref[span(i), span(j)], l_ref[span(i), span(j)] = split(x)
        if i != j:
            h_ref[span(j), span(i)], l_ref[span(j), span(i)] = split(jnp.transpose(x))

    def double_step(t_ref, th, tl, scale, x_ref):
        for i, j in pairs:
            at = (span(i), span(j))
            t2 = squared(th, tl, i, j)
            t = t_ref[at]
            if scale is not None:
                t2, t = (t2 * scale) * scale, t * scale
            put(ah, al, i, j, t2)
            put(bh, bl, i, j, 0.0625 * t2 - 0.5625 * t)
            x_ref[at] = 1.6875 * t2 - 2.4375 * t
        for i, j in pairs:
            at = (span(i), span(j))
            x_ref[at] = x_ref[at] + product(ah, al, bh, bl, i, j)

    double_step(s_ref, sh, sl, rescale, r_ref)
    for i, j in pairs:
        put(ah, al, i, j, r_ref[span(i), span(j)])
    for i, j in pairs:
        at = (span(i), span(j))
        put(bh, bl, i, j, 4.5 * r_ref[at] + squared(ah, al, i, j))
    for i, j in pairs:
        at = (span(i), span(j))
        q_ref[at] = (5.0625 * s_ref[at] + product(sh, sl, bh, bl, i, j)) * rescale
    for i, j in pairs:
        put(sh, sl, i, j, q_ref[span(i), span(j)])
    double_step(q_ref, sh, sl, None, q_ref)
    for i, j in pairs:
        put(ah, al, i, j, r_ref[span(i), span(j)])
        put(bh, bl, i, j, q_ref[span(i), span(j)])
    root = lax.rsqrt(fro)
    one = upper((TILE, TILE))[1]
    for i, j in pairs:
        at = (span(i), span(j))
        z = 2.25 * (r_ref[at] + q_ref[at]) + product(ah, al, bh, bl, i, j)
        if i == j:
            z = z + jnp.where(one, 5.0625, 0.0)
        w = (z * root).astype(BF16)
        w_ref[at] = w
        if i != j:
            w_ref[span(j), span(i)] = jnp.transpose(w.astype(F32)).astype(BF16)

    acc = jnp.zeros((TILE, TILE), F32)
    for i, j in pairs:
        g = dot(w_ref[span(i), :], w_ref[:, span(j)])
        acc = acc + g * s_ref[span(i), span(j)] * (1.0 if i == j else 2.0)
    trace = jnp.sum(jnp.sum(acc, axis=0, keepdims=True), axis=1, keepdims=True)
    en_ref[...] = trace * (1.0 / width)

    mean = jnp.concatenate(means, axis=1)
    for r in range(0, rows_dev, TILE):
        c = (e_ref[r : r + TILE, :].astype(F32) - mean).astype(BF16)
        o_ref[r : r + TILE, :] = dot(c, w_ref[...]).astype(BF16)


def groups(sizes):
    ny, nz, nx, _ = sizes

    def at(y, z, x, core):
        return ((y * nz + z) * nx + x) * 2 + core

    planes = [[at(y, z, x, 0) for y in range(ny) for x in range(nx)] for z in range(nz)]
    planes += [[at(y, z, x, 1) for z in range(nz) for x in range(nx)] for y in range(ny)]
    lines = [[at(y, z, x, 0) for z in range(nz)] for y in range(ny) for x in range(nx)]
    lines += [[at(y, z, x, 1) for y in range(ny)] for z in range(nz) for x in range(nx)]
    return planes, lines


def local(embeddings):
    rows_dev, width = embeddings.shape
    rows_total = rows_dev * lax.axis_size(AXES)
    sizes = [lax.axis_size(axis) for axis in AXES]
    _, _, _, need = layout(width)
    vmem = pl.BlockSpec(memory_space=pltpu.VMEM)

    planes, lines = groups(sizes)
    plane, line = len(planes[0]), len(lines[0])
    rows = -(-need // plane) * plane
    half_type = jax.ShapeDtypeStruct((rows, LANES), F32)

    def exchange(x, members):
        peers = len(members[0])
        y = x.reshape(peers, 1, x.shape[0] * LANES // peers)
        out = lax.all_to_all(y, AXES, 0, 0, axis_index_groups=members, tiled=True)
        return out.reshape(x.shape)

    def swap(x):
        return lax.ppermute(x, AXES[3], [(0, 1), (1, 0)])

    def call(kernel, out, name, *args, flops=0, mib=8, **rest):
        cost = pl.CostEstimate(flops=flops, bytes_accessed=0, transcendentals=0)
        return pl.pallas_call(
            kernel,
            out_shape=out,
            in_specs=[vmem] * len(args),
            out_specs=jax.tree.map(lambda _: vmem, out),
            cost_estimate=cost,
            compiler_params=pltpu.CompilerParams(vmem_limit_bytes=mib << 20),
            name=name,
            **rest,
        )(*args)

    flops = 2 * rows_dev * width * TILE
    theirs = swap(embeddings)
    own = call(gram_kernel, half_type, "gram_own", embeddings, flops=flops)
    packed = call(gram_kernel, half_type, "gram_both", theirs, own, flops=flops)

    def total(x, peers, copies):
        out = jax.ShapeDtypeStruct((x.shape[0] // peers * copies, LANES), F32)
        return call(functools.partial(total_kernel, peers, copies), out, f"total_{peers}_{copies}", x)

    x = total(exchange(packed, planes), plane, line)
    x = total(exchange(x, lines), line, plane)
    half = exchange(x, planes)
    square = (width, width)
    whitened, energy = call(
        functools.partial(whiten_kernel, rows_total),
        (jax.ShapeDtypeStruct((rows_dev, width), BF16), jax.ShapeDtypeStruct((1, 1), F32)),
        "whiten",
        embeddings,
        half,
        swap(half),
        flops=40 * width**3,
        mib=32,
        scratch_shapes=[pltpu.VMEM((2, rows, LANES), F32)]
        + [pltpu.VMEM(square, F32)] * 3
        + [pltpu.VMEM(square, BF16)] * 7,
    )
    return whitened, energy.reshape(())


def solution(mesh):
    torus = Mesh(mesh.devices.reshape(mesh.shape["grp"], 8, 4, 2), AXES)
    return jax.shard_map(
        local, mesh=torus, in_specs=(P(AXES, None),), out_specs=(P(AXES, None), P()), check_vma=False
    )
```

```python
import functools

import jax
import jax.numpy as jnp
from jax import lax
from jax.experimental import pallas as pl
from jax.experimental.pallas import tpu as pltpu
from jax.sharding import Mesh
from jax.sharding import PartitionSpec as P

ITERS = 4
AXES = ("grp", "row_0", "row_1", "row_2")
LANES = 128
TILE = 256
F32 = jnp.float32
BF16 = jnp.bfloat16


def layout(width):
    nb = width // LANES
    place = {}
    at = [0, 0]
    for i in range(nb):
        for j in range(i, nb):
            if j == i and i % 2:
                continue
            half = 0 if i < TILE // LANES and (i, j) != (1, nb - 1) else 1
            place[i, j] = (half, at[half])
            at[half] += LANES
    return nb, place, at[1], max(at[0], at[1] + nb + nb // 2)


def upper(shape):
    r = lax.broadcasted_iota(jnp.int32, shape, 0)
    c = lax.broadcasted_iota(jnp.int32, shape, 1)
    return r <= c, r == c


def gram_kernel(e_ref, *refs):
    o_ref = refs[-1]
    width = e_ref.shape[1]
    nb, place, tail, _ = layout(width)
    core = lax.axis_index(AXES[3])

    def put(at, rows):
        if len(refs) > 1:
            rows = rows + refs[0][at : at + rows.shape[0], :]
        o_ref[at : at + rows.shape[0], :] = rows

    def tile_row(big):
        keep, _ = upper((LANES, LANES))
        g = lax.dot_general(
            e_ref[:, big : big + TILE], e_ref[:, big:], (((0,), (0,)), ((), ())), preferred_element_type=F32
        )
        i = big // LANES

        def block(r, j):
            return g[r * LANES : (r + 1) * LANES, j * LANES - big : (j + 1) * LANES - big]

        put(place[i, i][1], jnp.where(keep, block(0, i), block(1, i + 1)))
        for r in range(2):
            for j in range(i + r + 1, nb):
                if (i + r, j) != (1, nb - 1):
                    put(place[i + r, j][1], block(r, j))

    @pl.when(core == 0)
    def _():
        tile_row(0)

    @pl.when(core == 1)
    def _():
        for big in range(TILE, width, TILE):
            tile_row(big)
        moved = lax.dot_general(
            e_ref[:, LANES:TILE], e_ref[:, width - LANES :], (((0,), (0,)), ((), ())), preferred_element_type=F32
        )
        put(place[1, nb - 1][1], moved)
        e = e_ref[...].astype(F32)
        colsum = jnp.sum(e, axis=0, keepdims=True)
        lines = [colsum[:, k * LANES : (k + 1) * LANES] for k in range(nb)]
        for k in range(1, nb, 2):
            x = e[:, k * LANES : (k + 1) * LANES]
            lines.append(jnp.sum(x * x, axis=0, keepdims=True))
        used = tail + len(lines)
        for k, line in enumerate(lines):
            put(tail + k, line)
        o_ref[used:, :] = jnp.zeros((o_ref.shape[0] - used, LANES), F32)


def total_kernel(peers, copies, x_ref, o_ref):
    rows = x_ref.shape[0] // peers
    acc = x_ref[:rows, :]
    for n in range(1, peers):
        acc = acc + x_ref[n * rows : (n + 1) * rows, :]
    for n in range(copies):
        o_ref[n * rows : (n + 1) * rows, :] = acc


def split(x):
    hi = x.astype(BF16)
    lo = (x - hi.astype(F32)).astype(BF16)
    return hi, lo


def whiten_kernel(rows_total, e_ref, own_ref, other_ref, o_ref, en_ref, half_ref, s_ref, r_ref, q_ref, sh, sl, ah, al, bh, bl, w_ref):
    rows_dev, width = e_ref.shape
    nb, place, tail, _ = layout(width)
    inv = 1.0 / rows_total
    keep, diag = upper((LANES, LANES))
    core = lax.axis_index(AXES[3])
    half_ref[core] = own_ref[...]
    half_ref[1 - core] = other_ref[...]

    def packed(i, j):
        half, at = place[i, j]
        return half_ref[half, at : at + LANES, :]

    def line(k):
        return half_ref[1, tail + k : tail + k + 1, :]

    means = [line(k) * inv for k in range(nb)]
    down = [jnp.transpose(jnp.broadcast_to(m, (LANES, LANES))) for m in means]

    squares = jnp.zeros((LANES, LANES), F32)
    for i in range(nb):
        for j in range(i, nb):
            if i != j:
                block = packed(i, j)
            else:
                base = i - i % 2
                both = packed(base, base)
                mirror = jnp.transpose(both)
                if i == base:
                    block = jnp.where(keep, both, mirror)
                else:
                    block = jnp.where(diag, line(nb + base // 2), jnp.where(keep, mirror, both))
            cov = block * inv - down[i] * means[j]
            squares = squares + (cov * cov) * (1.0 if i == j else 2.0)
            at = (slice(i * LANES, (i + 1) * LANES), slice(j * LANES, (j + 1) * LANES))
            s_ref[at] = cov
            sh[at], sl[at] = split(cov)
            if i != j:
                turned = jnp.transpose(cov)
                ta = (at[1], at[0])
                sh[ta], sl[ta] = split(turned)
                if i // (TILE // LANES) == j // (TILE // LANES):
                    s_ref[ta] = turned
    total = jnp.sum(jnp.sum(squares, axis=0, keepdims=True), axis=1, keepdims=True)
    fro = jnp.sqrt(total + 1e-06)
    rescale = 1.0 / fro

    nt = width // TILE
    pairs = [(i, j) for i in range(nt) for j in range(i, nt)]

    def span(i):
        return slice(i * TILE, (i + 1) * TILE)

    def dot(a, b):
        return jnp.dot(a, b, preferred_element_type=F32)

    def product(xh, xl, yh, yl, i, j):
        a, b = span(i), span(j)
        return dot(xh[a, :], yh[:, b]) + (dot(xh[a, :], yl[:, b]) + dot(xl[a, :], yh[:, b]))

    def squared(xh, xl, i, j):
        if i != j:
            return product(xh, xl, xh, xl, i, j)
        a = span(i)
        cross = dot(xh[a, :], xl[:, a])
        return dot(xh[a, :], xh[:, a]) + (cross + jnp.transpose(cross))

    def put(h_ref, l_ref, i, j, x):
        h_ref[span(i), span(j)], l_ref[span(i), span(j)] = split(x)
        if i != j:
            h_ref[span(j), span(i)], l_ref[span(j), span(i)] = split(jnp.transpose(x))

    def double_step(t_ref, th, tl, scale, x_ref):
        for i, j in pairs:
            at = (span(i), span(j))
            t2 = squared(th, tl, i, j)
            t = t_ref[at]
            if scale is not None:
                t2, t = (t2 * scale) * scale, t * scale
            v = t2 - 4.5 * t
            put(ah, al, i, j, v)
            x_ref[at] = 0.421875 * v - 0.5390625 * t
        for i, j in pairs:
            at = (span(i), span(j))
            x_ref[at] = x_ref[at] + 0.0625 * squared(ah, al, i, j)

    double_step(s_ref, sh, sl, rescale, r_ref)
    for i, j in pairs:
        put(ah, al, i, j, r_ref[span(i), span(j)])
    for i, j in pairs:
        at = (span(i), span(j))
        put(bh, bl, i, j, 4.5 * r_ref[at] + squared(ah, al, i, j))
    for i, j in pairs:
        at = (span(i), span(j))
        q_ref[at] = (5.0625 * s_ref[at] + product(sh, sl, bh, bl, i, j)) * rescale
    for i, j in pairs:
        put(sh, sl, i, j, q_ref[span(i), span(j)])
    double_step(q_ref, sh, sl, None, q_ref)
    for i, j in pairs:
        put(ah, al, i, j, r_ref[span(i), span(j)])
        put(bh, bl, i, j, q_ref[span(i), span(j)])
    root = lax.rsqrt(fro)
    one = upper((TILE, TILE))[1]
    for i, j in pairs:
        at = (span(i), span(j))
        z = 2.25 * (r_ref[at] + q_ref[at]) + product(ah, al, bh, bl, i, j)
        if i == j:
            z = z + jnp.where(one, 5.0625, 0.0)
        w = (z * root).astype(BF16)
        w_ref[at] = w
        if i != j:
            w_ref[span(j), span(i)] = jnp.transpose(w.astype(F32)).astype(BF16)

    acc = jnp.zeros((TILE, TILE), F32)
    for i, j in pairs:
        g = dot(w_ref[span(i), :], w_ref[:, span(j)])
        acc = acc + g * s_ref[span(i), span(j)] * (1.0 if i == j else 2.0)
    trace = jnp.sum(jnp.sum(acc, axis=0, keepdims=True), axis=1, keepdims=True)
    en_ref[...] = trace * (1.0 / width)

    mean = jnp.concatenate(means, axis=1)
    for r in range(0, rows_dev, TILE):
        c = (e_ref[r : r + TILE, :].astype(F32) - mean).astype(BF16)
        o_ref[r : r + TILE, :] = dot(c, w_ref[...]).astype(BF16)


def groups(sizes):
    ny, nz, nx, _ = sizes

    def at(y, z, x, core):
        return ((y * nz + z) * nx + x) * 2 + core

    planes = [[at(y, z, x, 0) for y in range(ny) for x in range(nx)] for z in range(nz)]
    planes += [[at(y, z, x, 1) for z in range(nz) for x in range(nx)] for y in range(ny)]
    lines = [[at(y, z, x, 0) for z in range(nz)] for y in range(ny) for x in range(nx)]
    lines += [[at(y, z, x, 1) for y in range(ny)] for z in range(nz) for x in range(nx)]
    return planes, lines


def local(embeddings):
    rows_dev, width = embeddings.shape
    rows_total = rows_dev * lax.axis_size(AXES)
    sizes = [lax.axis_size(axis) for axis in AXES]
    _, _, _, need = layout(width)
    vmem = pl.BlockSpec(memory_space=pltpu.VMEM)

    planes, lines = groups(sizes)
    plane, line = len(planes[0]), len(lines[0])
    rows = -(-need // plane) * plane
    half_type = jax.ShapeDtypeStruct((rows, LANES), F32)

    def exchange(x, members):
        peers = len(members[0])
        y = x.reshape(peers, 1, x.shape[0] * LANES // peers)
        out = lax.all_to_all(y, AXES, 0, 0, axis_index_groups=members, tiled=True)
        return out.reshape(x.shape)

    def swap(x):
        return lax.ppermute(x, AXES[3], [(0, 1), (1, 0)])

    def call(kernel, out, name, *args, flops=0, mib=8, **rest):
        cost = pl.CostEstimate(flops=flops, bytes_accessed=0, transcendentals=0)
        return pl.pallas_call(
            kernel,
            out_shape=out,
            in_specs=[vmem] * len(args),
            out_specs=jax.tree.map(lambda _: vmem, out),
            cost_estimate=cost,
            compiler_params=pltpu.CompilerParams(vmem_limit_bytes=mib << 20),
            name=name,
            **rest,
        )(*args)

    flops = 2 * rows_dev * width * TILE
    theirs = swap(embeddings)
    own = call(gram_kernel, half_type, "gram_own", embeddings, flops=flops)
    packed = call(gram_kernel, half_type, "gram_both", theirs, own, flops=flops)

    def total(x, peers, copies):
        out = jax.ShapeDtypeStruct((x.shape[0] // peers * copies, LANES), F32)
        return call(functools.partial(total_kernel, peers, copies), out, f"total_{peers}_{copies}", x)

    x = total(exchange(packed, planes), plane, line)
    x = total(exchange(x, lines), line, plane)
    half = exchange(x, planes)
    square = (width, width)
    whitened, energy = call(
        functools.partial(whiten_kernel, rows_total),
        (jax.ShapeDtypeStruct((rows_dev, width), BF16), jax.ShapeDtypeStruct((1, 1), F32)),
        "whiten",
        embeddings,
        half,
        swap(half),
        flops=40 * width**3,
        mib=32,
        scratch_shapes=[pltpu.VMEM((2, rows, LANES), F32)]
        + [pltpu.VMEM(square, F32)] * 3
        + [pltpu.VMEM(square, BF16)] * 7,
    )
    return whitened, energy.reshape(())


def solution(mesh):
    torus = Mesh(mesh.devices.reshape(mesh.shape["grp"], 8, 4, 2), AXES)
    return jax.shard_map(
        local, mesh=torus, in_specs=(P(AXES, None),), out_specs=(P(AXES, None), P()), check_vma=False
    )
```

```python
import functools

import jax
import jax.numpy as jnp
from jax import lax
from jax.experimental import pallas as pl
from jax.experimental.pallas import tpu as pltpu
from jax.sharding import Mesh
from jax.sharding import PartitionSpec as P

ITERS = 4
AXES = ("grp", "row_0", "row_1", "row_2")
LANES = 128
TILE = 256
F32 = jnp.float32
BF16 = jnp.bfloat16


def layout(width):
    nb = width // LANES
    place = {}
    at = [0, 0]
    for i in range(nb):
        for j in range(i, nb):
            if j == i and i % 2:
                continue
            half = 0 if i < TILE // LANES and (i, j) != (1, nb - 1) else 1
            place[i, j] = (half, at[half])
            at[half] += LANES
    return nb, place, at[1], max(at[0], at[1] + nb + nb // 2)


def upper(shape):
    r = lax.broadcasted_iota(jnp.int32, shape, 0)
    c = lax.broadcasted_iota(jnp.int32, shape, 1)
    return r <= c, r == c


def gram_kernel(e_ref, *refs):
    o_ref = refs[-1]
    width = e_ref.shape[1]
    nb, place, tail, _ = layout(width)
    core = lax.axis_index(AXES[3])

    def put(at, rows):
        if len(refs) > 1:
            rows = rows + refs[0][at : at + rows.shape[0], :]
        o_ref[at : at + rows.shape[0], :] = rows

    def tile_row(big):
        keep, _ = upper((LANES, LANES))
        g = lax.dot_general(
            e_ref[:, big : big + TILE], e_ref[:, big:], (((0,), (0,)), ((), ())), preferred_element_type=F32
        )
        i = big // LANES

        def block(r, j):
            return g[r * LANES : (r + 1) * LANES, j * LANES - big : (j + 1) * LANES - big]

        put(place[i, i][1], jnp.where(keep, block(0, i), block(1, i + 1)))
        for r in range(2):
            for j in range(i + r + 1, nb):
                if (i + r, j) != (1, nb - 1):
                    put(place[i + r, j][1], block(r, j))

    @pl.when(core == 0)
    def _():
        tile_row(0)

    @pl.when(core == 1)
    def _():
        for big in range(TILE, width, TILE):
            tile_row(big)
        moved = lax.dot_general(
            e_ref[:, LANES:TILE], e_ref[:, width - LANES :], (((0,), (0,)), ((), ())), preferred_element_type=F32
        )
        put(place[1, nb - 1][1], moved)
        e = e_ref[...].astype(F32)
        colsum = jnp.sum(e, axis=0, keepdims=True)
        lines = [colsum[:, k * LANES : (k + 1) * LANES] for k in range(nb)]
        for k in range(1, nb, 2):
            x = e[:, k * LANES : (k + 1) * LANES]
            lines.append(jnp.sum(x * x, axis=0, keepdims=True))
        used = tail + len(lines)
        for k, line in enumerate(lines):
            put(tail + k, line)
        o_ref[used:, :] = jnp.zeros((o_ref.shape[0] - used, LANES), F32)


def total_kernel(peers, copies, x_ref, o_ref):
    rows = x_ref.shape[0] // peers
    acc = x_ref[:rows, :]
    for n in range(1, peers):
        acc = acc + x_ref[n * rows : (n + 1) * rows, :]
    for n in range(copies):
        o_ref[n * rows : (n + 1) * rows, :] = acc


def split(x):
    hi = x.astype(BF16)
    lo = (x - hi.astype(F32)).astype(BF16)
    return hi, lo


def whiten_kernel(rows_total, e_ref, own_ref, other_ref, o_ref, en_ref, half_ref, s_ref, r_ref, q_ref, sh, sl, ah, al, bh, bl, w_ref, white_ref, sems):
    rows_dev, width = e_ref.shape
    nb, place, tail, _ = layout(width)
    inv = 1.0 / rows_total
    keep, diag = upper((LANES, LANES))
    core = lax.axis_index(AXES[3])
    half_ref[core] = own_ref[...]
    half_ref[1 - core] = other_ref[...]

    def packed(i, j):
        half, at = place[i, j]
        return half_ref[half, at : at + LANES, :]

    def line(k):
        return half_ref[1, tail + k : tail + k + 1, :]

    means = [line(k) * inv for k in range(nb)]
    down = [jnp.transpose(jnp.broadcast_to(m, (LANES, LANES))) for m in means]

    squares = jnp.zeros((LANES, LANES), F32)
    for i in range(nb):
        for j in range(i, nb):
            if i != j:
                block = packed(i, j)
            else:
                base = i - i % 2
                both = packed(base, base)
                mirror = jnp.transpose(both)
                if i == base:
                    block = jnp.where(keep, both, mirror)
                else:
                    block = jnp.where(diag, line(nb + base // 2), jnp.where(keep, mirror, both))
            cov = block * inv - down[i] * means[j]
            squares = squares + (cov * cov) * (1.0 if i == j else 2.0)
            at = (slice(i * LANES, (i + 1) * LANES), slice(j * LANES, (j + 1) * LANES))
            s_ref[at] = cov
            sh[at], sl[at] = split(cov)
            if i != j:
                ta = (at[1], at[0])
                sh[ta], sl[ta] = jnp.transpose(sh[at]), jnp.transpose(sl[at])
                if i // (TILE // LANES) == j // (TILE // LANES):
                    s_ref[ta] = jnp.transpose(cov)
    total = jnp.sum(jnp.sum(squares, axis=0, keepdims=True), axis=1, keepdims=True)
    fro = jnp.sqrt(total + 1e-06)
    rescale = 1.0 / fro

    nt = width // TILE
    pairs = [(i, j) for i in range(nt) for j in range(i, nt)]

    def span(i):
        return slice(i * TILE, (i + 1) * TILE)

    def dot(a, b):
        return jnp.dot(a, b, preferred_element_type=F32)

    def product(xh, xl, yh, yl, i, j):
        a, b = span(i), span(j)
        return dot(xh[a, :], yh[:, b]) + (dot(xh[a, :], yl[:, b]) + dot(xl[a, :], yh[:, b]))

    def squared(xh, xl, i, j):
        if i != j:
            return product(xh, xl, xh, xl, i, j)
        a = span(i)
        cross = dot(xh[a, :], xl[:, a])
        return dot(xh[a, :], xh[:, a]) + (cross + jnp.transpose(cross))

    def put(h_ref, l_ref, i, j, x):
        hi, lo = split(x)
        h_ref[span(i), span(j)], l_ref[span(i), span(j)] = hi, lo
        if i != j:
            h_ref[span(j), span(i)], l_ref[span(j), span(i)] = jnp.transpose(hi), jnp.transpose(lo)

    def double_step(t_ref, th, tl, scale, x_ref):
        for i, j in pairs:
            at = (span(i), span(j))
            t2 = squared(th, tl, i, j)
            t = t_ref[at]
            if scale is not None:
                t2, t = (t2 * scale) * scale, t * scale
            v = t2 - 4.5 * t
            put(ah, al, i, j, v)
            x_ref[at] = 0.421875 * v - 0.5390625 * t
        for i, j in pairs:
            at = (span(i), span(j))
            x_ref[at] = x_ref[at] + 0.0625 * squared(ah, al, i, j)

    double_step(s_ref, sh, sl, rescale, r_ref)
    for i, j in pairs:
        put(ah, al, i, j, r_ref[span(i), span(j)])
    for i, j in pairs:
        at = (span(i), span(j))
        put(bh, bl, i, j, 4.5 * r_ref[at] + squared(ah, al, i, j))
    for i, j in pairs:
        at = (span(i), span(j))
        q_ref[at] = (5.0625 * s_ref[at] + product(sh, sl, bh, bl, i, j)) * rescale
    for i, j in pairs:
        put(sh, sl, i, j, q_ref[span(i), span(j)])
    double_step(q_ref, sh, sl, None, q_ref)
    for i, j in pairs:
        put(ah, al, i, j, r_ref[span(i), span(j)])
        put(bh, bl, i, j, q_ref[span(i), span(j)])
    root = lax.rsqrt(fro)
    one = upper((TILE, TILE))[1]
    for i, j in pairs:
        at = (span(i), span(j))
        z = 2.25 * (r_ref[at] + q_ref[at]) + product(ah, al, bh, bl, i, j)
        if i == j:
            z = z + jnp.where(one, 5.0625, 0.0)
        w = (z * root).astype(BF16)
        w_ref[at] = w
        if i != j:
            w_ref[span(j), span(i)] = jnp.transpose(w)

    mean = jnp.concatenate(means, axis=1)
    copies = []
    for n, r in enumerate(range(0, rows_dev, LANES)):
        c = (e_ref[r : r + LANES, :].astype(F32) - mean).astype(BF16)
        white_ref[r : r + LANES, :] = dot(c, w_ref[...]).astype(BF16)
        if copies:
            copies[-1].start()
        piece = pl.ds(r, LANES)
        copies.append(pltpu.make_async_copy(white_ref.at[piece, :], o_ref.at[piece, :], sems.at[n]))

    acc = jnp.zeros((TILE, TILE), F32)
    for n, (i, j) in enumerate(pairs):
        g = dot(w_ref[span(i), :], w_ref[:, span(j)])
        acc = acc + g * s_ref[span(i), span(j)] * (1.0 if i == j else 2.0)
        if n == 0:
            copies[-1].start()
    trace = jnp.sum(jnp.sum(acc, axis=0, keepdims=True), axis=1, keepdims=True)
    en_ref[...] = trace * (1.0 / width)
    for copy in copies:
        copy.wait()


def groups(sizes):
    ny, nz, nx, _ = sizes

    def at(y, z, x, core):
        return ((y * nz + z) * nx + x) * 2 + core

    planes = [[at(y, z, x, 0) for y in range(ny) for x in range(nx)] for z in range(nz)]
    planes += [[at(y, z, x, 1) for z in range(nz) for x in range(nx)] for y in range(ny)]
    lines = [[at(y, z, x, 0) for z in range(nz)] for y in range(ny) for x in range(nx)]
    lines += [[at(y, z, x, 1) for y in range(ny)] for z in range(nz) for x in range(nx)]
    return planes, lines


def local(embeddings):
    rows_dev, width = embeddings.shape
    rows_total = rows_dev * lax.axis_size(AXES)
    sizes = [lax.axis_size(axis) for axis in AXES]
    _, _, _, need = layout(width)
    vmem = pl.BlockSpec(memory_space=pltpu.VMEM)

    planes, lines = groups(sizes)
    plane, line = len(planes[0]), len(lines[0])
    rows = -(-need // plane) * plane
    half_type = jax.ShapeDtypeStruct((rows, LANES), F32)

    def exchange(x, members):
        peers = len(members[0])
        y = x.reshape(peers, 1, x.shape[0] * LANES // peers)
        out = lax.all_to_all(y, AXES, 0, 0, axis_index_groups=members, tiled=True)
        return out.reshape(x.shape)

    def swap(x):
        return lax.ppermute(x, AXES[3], [(0, 1), (1, 0)])

    def call(kernel, out, name, *args, flops=0, mib=8, out_specs=None, **rest):
        cost = pl.CostEstimate(flops=flops, bytes_accessed=0, transcendentals=0)
        return pl.pallas_call(
            kernel,
            out_shape=out,
            in_specs=[vmem] * len(args),
            out_specs=out_specs or jax.tree.map(lambda _: vmem, out),
            cost_estimate=cost,
            compiler_params=pltpu.CompilerParams(vmem_limit_bytes=mib << 20),
            name=name,
            **rest,
        )(*args)

    flops = 2 * rows_dev * width * TILE
    theirs = swap(embeddings)
    own = call(gram_kernel, half_type, "gram_own", embeddings, flops=flops)
    packed = call(gram_kernel, half_type, "gram_both", theirs, own, flops=flops)

    def total(x, peers, copies):
        out = jax.ShapeDtypeStruct((x.shape[0] // peers * copies, LANES), F32)
        return call(functools.partial(total_kernel, peers, copies), out, f"total_{peers}_{copies}", x)

    x = total(exchange(packed, planes), plane, line)
    x = total(exchange(x, lines), line, plane)
    half = exchange(x, planes)
    square = (width, width)
    whitened, energy = call(
        functools.partial(whiten_kernel, rows_total),
        (jax.ShapeDtypeStruct((rows_dev, width), BF16), jax.ShapeDtypeStruct((1, 1), F32)),
        "whiten",
        embeddings,
        half,
        swap(half),
        flops=40 * width**3,
        mib=32,
        out_specs=(pl.BlockSpec(memory_space=pl.ANY), vmem),
        scratch_shapes=[pltpu.VMEM((2, rows, LANES), F32)]
        + [pltpu.VMEM(square, F32)] * 3
        + [pltpu.VMEM(square, BF16)] * 7
        + [pltpu.VMEM((rows_dev, width), BF16), pltpu.SemaphoreType.DMA((rows_dev // LANES,))],
    )
    return whitened, energy.reshape(())


def solution(mesh):
    torus = Mesh(mesh.devices.reshape(mesh.shape["grp"], 8, 4, 2), AXES)
    return jax.shard_map(
        local, mesh=torus, in_specs=(P(AXES, None),), out_specs=(P(AXES, None), P()), check_vma=False
    )
```
